128 devices in a mesh: tp: 16 (over z, x_hi, core), fs: 8 (over y, x_lo).
Axes of the slice: x: 4 (x_hi: 2, x_lo: 2; x = x_hi * 2 + x_lo), y: 4, z: 4, core: 2. Of those that a mesh axis runs over, the one named last changes fastest.
Arguments:
- tokens: bfloat16 [512, 8192], P(('tp', 'fs')), may hold values from -6 to 6
- gate_weight: bfloat16 [8192, 29568], P('fs', 'tp'), may hold values from -0.0625 to 0.0625
- up_weight: bfloat16 [8192, 29568], P('fs', 'tp'), may hold values from -0.0625 to 0.0625
- down_weight: bfloat16 [29568, 8192], P('tp', 'fs'), may hold values from -0.046875 to 0.046875
Outputs:
- mixed: bfloat16 [512, 8192], P(None, ('fs', 'tp'))
The draws below stay inside these ranges and needn't reach their ends.
All inputs are finite; a program needn't handle non-finite values.
Results may differ from the reference program's by a relative error of at most 0.0049.
Values may be sent and summed in bfloat16 or wider, within the bound.
A program may use at most 64 MiB of HBM per device.

```python
import jax
import jax.numpy as jnp

D = 8192
FF = 29568
TOKENS = 512


def strengthened(values, key, source, target, shards_of, factor):
    owner, partner = [(jnp.arange(values.shape[dim]) // (values.shape[dim] // shards_of)).reshape([-1 if axis == dim else 1 for axis in range(values.ndim)]) for dim in (source, target)]
    chosen = jax.random.permutation(key, shards_of)[partner]
    strong = (owner == chosen) | (owner == (partner + shards_of // 2) % shards_of)
    return jnp.where(strong, factor * values, values)


def shard_levels(own_key, shape, pieces, low, high):
    def one(dim, blocks):
        draws = jax.random.uniform(jax.random.fold_in(jax.random.fold_in(own_key, 6), dim), (blocks,), jnp.float32, low / len(pieces), high / len(pieces))
        return jnp.repeat(jnp.exp(draws), shape[dim] // blocks).reshape((-1,) + (1,) * (len(shape) - dim - 1))

    level = one(*pieces[0])
    for cut in pieces[1:]:
        level = level * one(*cut)
    return level


def bell_draw(own_key, extent, spread, bound, pieces=(), held_as=jnp.bfloat16):
    loudness = shard_levels(own_key, extent, pieces, -0.22, 0.18) if pieces else 1.0
    entries = jax.random.normal(own_key, extent, jnp.float32) * spread * loudness
    return jnp.minimum(jnp.maximum(entries, -bound), bound).astype(held_as)


def gaussian_with(own_key, shape, width, most, split, heavy, kind=jnp.bfloat16):
    array = width * jax.random.normal(own_key, shape, jnp.float32)
    if split:
        array = array * shard_levels(own_key, shape, split, -0.22, 0.18)
    return jnp.clip(strengthened(array, jax.random.fold_in(own_key, 3), *heavy), -most, most).astype(kind)


def setup_inputs(seed: int = 0) -> dict:
    key_list = jax.random.split(jax.random.key(seed), 5)
    tokens = bell_draw(key_list[0], (TOKENS, D), 1.0, 6.0, ((0, 128),))
    gate_weight = bell_draw(key_list[1], (D, FF), D ** -0.5, 0.0625, ((0, 8), (1, 16)))
    up_weight = bell_draw(key_list[2], (D, FF), D ** -0.5, 0.0625, ((0, 8), (1, 16)))
    down_weight = gaussian_with(key_list[3], (FF, D), FF ** -0.5, 0.046875, ((0, 16), (1, 8)), (0, 1, 16, 2.0))
    return dict(tokens=tokens, gate_weight=gate_weight, up_weight=up_weight, down_weight=down_weight)


def reference(tokens, gate_weight, up_weight, down_weight):
    gate = jnp.dot(tokens, gate_weight, preferred_element_type=jnp.float32)
    up = jnp.dot(tokens, up_weight, preferred_element_type=jnp.float32)
    hidden = (jax.nn.silu(gate) * up).astype(jnp.bfloat16)
    mixed = jnp.dot(hidden, down_weight, preferred_element_type=jnp.float32)
    return mixed.astype(jnp.bfloat16)
```

```python
import functools

import jax
import jax.numpy as jnp
from jax import lax
from jax.experimental import pallas as pl
from jax.experimental.pallas import tpu as pltpu
from jax.sharding import PartitionSpec as P

BF = jnp.bfloat16
F32 = jnp.float32
MESH = pl.DeviceIdType.MESH

FAR, EARLY, LATE, XS, HY, HF, HX, DD = 0, 2, 4, 6, 7, 9, 11, 15
SPLIT = 1024
PLAN = (
    "M0 A0 B0 M1",
    "A1 C0 B1 D0",
    "M2 A2 E0 C1",
    "B2 F0 D1 M3",
    "A3 E1 G0 C2",
    "B3 I0 F1 D2",
    "G1 E2 C3 I1",
    "F2 D3 G2 E3",
    "I2 F3 G3 I3",
)


def kernel(tok, wg_hbm, wu_hbm, wd_hbm, out, wg, wu, wd, slab, x, pf, sf, far_s, far_r, early_s, early_r,
           late_s, late_r, xs_s, xs_r, keep, hb, mf, dd_s, dd_r, mb, mr, own, fin_s, fin_r,
           wsem, t1s, t1r, t2s, t2r, zs, zr, rs, rr, ms, mrs, fs_sem, fr_sem):
    f = lax.axis_index("fs")
    t = lax.axis_index("tp")
    y, xl = f // 2, f % 2
    z, xh, core = t // 4, (t // 2) % 2, t % 2
    chip = t // 2
    ff = pf.shape[-1]

    def fs_dev(yy, xx):
        return {"fs": (yy % 4) * 2 + xx, "tp": t}

    def tp_dev(zz, hh, cc):
        return {"fs": f, "tp": (zz % 4) * 4 + hh * 2 + cc}

    loads = [pltpu.make_async_copy(a, b, wsem.at[i]) for i, (a, b) in enumerate(((wg_hbm, wg), (wu_hbm, wu), (wd_hbm, wd)))]
    for c in loads:
        c.start()

    ydev = (fs_dev(y + 1, xl), fs_dev(y + 3, xl))
    xdev = fs_dev(y, 1 - xl)
    cdev = tp_dev(z, xh, 1 - core)
    zdev = (tp_dev(z + 1, xh, core), tp_dev(z + 3, xh, core))
    fs_all = [{"fs": (f + k) % 8, "tp": t} for k in range(1, 8)]
    chips = [{"fs": f, "tp": ((chip + k) % 8) * 2 + core} for k in range(1, 8)]
    block = [cdev, tp_dev(z, 1 - xh, core), tp_dev(z, 1 - xh, 1 - core)]

    barrier = pltpu.get_barrier_semaphore()
    peers = fs_all + chips + [block[0], block[2]]
    for d in peers:
        pl.semaphore_signal(barrier, inc=1, device_id=d, device_id_type=MESH)
    pl.semaphore_wait(barrier, len(peers))

    sent = []

    def send(src, dst, ssem, rsem, dev):
        c = pltpu.make_async_remote_copy(src_ref=src, dst_ref=dst, send_sem=ssem, recv_sem=rsem, device_id=dev, device_id_type=MESH)
        c.start()
        sent.append(c)
        return c

    t1 = []
    for k in range(1, 8):
        g = (f + k) % 8
        cols = pl.ds(pl.multiple_of(g * 1024, 1024), 1024)
        t1.append(send(tok.at[:, cols], slab.at[f], t1s.at[k - 1], t1r.at[k - 1], fs_all[k - 1]))
    slab[f] = tok[:, pl.ds(pl.multiple_of(f * 1024, 1024), 1024)]
    for c in t1:
        c.wait_recv()
    quarter = xh * 2 + core
    rows32 = pl.ds(pl.multiple_of(quarter * 32, 32), 32)
    x[z, rows32, :] = slab[...].astype(F32).reshape(32, 1024).astype(BF)
    t2 = [send(x.at[z, rows32], x.at[z, rows32], t2s.at[k], t2r.at[k], block[k]) for k in range(3)]

    zb = (z, (z + 3) % 4, (z + 1) % 4, (z + 2) % 4)
    r32 = lambda yy: pl.ds(pl.multiple_of((yy % 4) * 32, 32), 32)
    r16 = lambda yy, xx: pl.ds(pl.multiple_of((yy % 4) * 32 + xx * 16, 16), 16)
    zc = {}

    def M(i):
        if i == 0:
            for c in t2:
                c.wait_recv()
            zc[0] = send(x.at[z], x.at[z], zs.at[0], zr.at[0], zdev[0])
            zc[1] = send(x.at[z], x.at[z], zs.at[1], zr.at[1], zdev[1])
            loads[0].wait()
            loads[1].wait()
        elif i == 1:
            zc[0].wait_recv()
            half = x.at[zb[1], pl.ds(0, 64)]
            zc[2] = send(half, half, zs.at[2], zr.at[2], zdev[0])
        elif i == 2:
            zc[1].wait_recv()
            half = x.at[zb[2], pl.ds(64, 64)]
            zc[3] = send(half, half, zs.at[3], zr.at[3], zdev[1])
        else:
            zc[2].wait_recv()
            zc[3].wait_recv()
        xi = x[zb[i]]
        pf[i, 0] = jnp.dot(xi, wg[...], preferred_element_type=F32)
        pf[i, 1] = jnp.dot(xi, wu[...], preferred_element_type=F32)

    rc = {}

    def rsend(i, k, src, dst, dev):
        rc[i, k] = send(src, dst, rs.at[i, k], rr.at[i, k], dev)

    def A(i):
        for d in (0, 1):
            far_s[i, d] = pf[i, :, r16(y + 2, d), :].astype(BF)
            rsend(i, FAR + d, far_s.at[i, d], far_r.at[i, d], ydev[d])
        for d in (0, 1):
            early_s[i, d] = pf[i, :, r16(y + 1 + 2 * d, 1 - d), :].astype(BF)
            rsend(i, EARLY + d, early_s.at[i, d], early_r.at[i, d], ydev[d])

    def B(i):
        for d in (0, 1):
            rc[i, FAR + d].wait_recv()
            late_s[i, d] = (pf[i, :, r16(y + 1 + 2 * d, d), :] + far_r[i, d].astype(F32)).astype(BF)
            rsend(i, LATE + d, late_s.at[i, d], late_r.at[i, d], ydev[d])

    def C(i):
        for k in (EARLY, EARLY + 1, LATE, LATE + 1):
            rc[i, k].wait_recv()
        sf[0] = pf[i, :, r16(y, 0), :] + late_r[i, 0].astype(F32) + early_r[i, 1].astype(F32)
        sf[1] = pf[i, :, r16(y, 1), :] + early_r[i, 0].astype(F32) + late_r[i, 1].astype(F32)
        xs_s[i] = sf[1 - xl].astype(BF)
        rsend(i, XS, xs_s.at[i], xs_r.at[i], xdev)
        keep[i] = sf[xl]

    def hrow(i, yy, xx):
        return hb.at[i, r16(yy, xx)]

    def D(i):
        rc[i, XS].wait_recv()
        gu = keep[i] + xs_r[i].astype(F32)
        g, u = gu[0], gu[1]
        hb[i, r16(y, xl), :] = (g / (1.0 + jnp.exp(-g)) * u).astype(BF)
        piece = hrow(i, y, xl)
        rsend(i, HY, piece, piece, ydev[0])
        rsend(i, HY + 1, piece, piece, ydev[1])
        rsend(i, HX, piece, piece, xdev)

    def E(i):
        for d in (0, 1):
            rc[i, HY + d].wait_recv()
            yy = y + 3 - 2 * d
            cols = pl.ds(0, SPLIT) if d == 0 else pl.ds(SPLIT, ff - SPLIT)
            part = hb.at[i, r16(yy, xl), cols]
            rsend(i, HF + d, part, part, ydev[d])
            piece = hrow(i, yy, xl)
            rsend(i, HX + 1 + d, piece, piece, xdev)

    def F(i):
        rc[i, HF].wait_recv()
        rc[i, HF + 1].wait_recv()
        piece = hrow(i, y + 2, xl)
        rsend(i, HX + 3, piece, piece, xdev)

    def G(i):
        if i == 0:
            loads[2].wait()
        for k in range(4):
            rc[i, HX + k].wait_recv()
        mf[i] = jnp.dot(hb[i], wd[...], preferred_element_type=F32)
        dd_s[i] = mf[i, pl.ds(pl.multiple_of((1 - core) * 64, 64), 64), :]
        rsend(i, DD, dd_s.at[i], dd_r.at[i], cdev)

    mc = {}

    def I(i):
        rc[i, DD].wait_recv()
        s = mf[i, pl.ds(pl.multiple_of(core * 64, 64), 64), :] + dd_r[i]
        mf[i, :64, :] = s
        mb[i] = s.astype(BF)
        own[zb[i]] = mf[i, :64, pl.ds(pl.multiple_of(chip * 128, 128), 128)]
        for k in range(1, 8):
            g = (chip + k) % 8
            cols = pl.ds(pl.multiple_of(g * 128, 128), 128)
            mc[i, k] = send(mb.at[i, :, cols], mr.at[zb[i], chip], ms.at[i, k], mrs.at[zb[i], chip], chips[k - 1])

    ops = dict(M=M, A=A, B=B, C=C, D=D, E=E, F=F, G=G, I=I)
    for step in " ".join(PLAN).split():
        ops[step[0]](int(step[1:]))

    for b in range(4):
        total = own[b]
        for k in range(1, 8):
            g = (chip + k) % 8
            pltpu.make_async_remote_copy(src_ref=mr.at[b, g], dst_ref=mr.at[b, g], send_sem=ms.at[b, k], recv_sem=mrs.at[b, g],
                                         device_id=chips[k - 1], device_id_type=MESH).wait_recv()
            total = total + mr[b, g].astype(F32)
        fin_s[b] = total.astype(BF)
    fc = send(fin_s, fin_r, fs_sem, fr_sem, cdev)

    def place(v, which):
        for b in range(4):
            vb = v[b]
            sel = jnp.where(core == 0, vb[:, :64].astype(F32), vb[:, 64:].astype(F32)).astype(BF)
            out[pl.ds(pl.multiple_of(b * 128 + which * 64, 64), 64), :] = sel

    place(fin_s, core)
    fc.wait_recv()
    place(fin_r, 1 - core)
    for c in sent:
        c.wait_send()


def body(tokens, gate_weight, up_weight, down_weight):
    d, ff = gate_weight.shape
    vm = pltpu.VMEM
    sem = lambda *s: pltpu.SemaphoreType.DMA(s) if s else pltpu.SemaphoreType.DMA
    piece = lambda: vm((4, 2, 2, 16, ff), BF)
    scratch = [
        vm((d, ff), BF), vm((d, ff), BF), vm((ff, d), BF), vm((8, 4, 1024), BF), vm((4, 128, 1024), BF),
        vm((4, 2, 128, ff), F32), vm((2, 2, 16, ff), F32), piece(), piece(), piece(), piece(), piece(), piece(),
        vm((4, 2, 16, ff), BF), vm((4, 2, 16, ff), BF), vm((4, 2, 16, ff), F32), vm((4, 128, ff), BF),
        vm((4, 128, 1024), F32), vm((4, 64, 1024), F32), vm((4, 64, 1024), F32), vm((4, 64, 1024), BF),
        vm((4, 8, 64, 128), BF), vm((4, 64, 128), F32), vm((4, 64, 128), BF), vm((4, 64, 128), BF),
        sem(3), sem(7), sem(7), sem(3), sem(3), sem(4), sem(4), sem(4, 16), sem(4, 16), sem(4, 8), sem(4, 8),
        sem(), sem(),
    ]
    return pl.pallas_call(
        kernel,
        out_shape=jax.ShapeDtypeStruct((512, 64), BF),
        in_specs=[pl.BlockSpec(memory_space=vm)] + [pl.BlockSpec(memory_space=pl.ANY)] * 3,
        out_specs=pl.BlockSpec(memory_space=vm),
        scratch_shapes=scratch,
        compiler_params=pltpu.CompilerParams(collective_id=0, has_side_effects=True, vmem_limit_bytes=60 * 2**20),
        name="ffn",
    )(tokens, gate_weight, up_weight, down_weight)


def solution(mesh):
    in_specs = (P(("tp", "fs"), None), P("fs", "tp"), P("fs", "tp"), P("tp", "fs"))
    out_specs = P(None, ("fs", "tp"))
    return jax.shard_map(body, mesh=mesh, in_specs=in_specs, out_specs=out_specs, check_vma=False)
```

```python
import functools

import jax
import jax.numpy as jnp
from jax import lax
from jax.experimental import pallas as pl
from jax.experimental.pallas import tpu as pltpu
from jax.sharding import PartitionSpec as P

BF = jnp.bfloat16
F32 = jnp.float32
MESH = pl.DeviceIdType.MESH

(UF, UE, UL, UX, GX, GF, GE, GL, AX, AY, AP, AQ, AF, AR, DD) = (0, 2, 4, 6, 7, 11, 13, 15, 17, 18, 20, 22, 24, 26, 30)
GL_COLS = 896
P_COLS = 1280
Q_COLS = 1536
PLAN = (
    "t0 g0 u0 r1",
    "r0 b0 g2 c0",
    "u1 f0 u2 g3",
    "d0 c2 w0 b1",
    "e0 g1 b2 u3",
    "e2 d2 b3 h0",
    "c3 c1 d1 e3",
    "h2 e1 d3 i0",
    "i2 h3 j0 h1",
    "j2 i3 i1 k2",
    "j3 k0 j1 l2",
    "l0 k3 k1 l3",
    "l1",
)


def dot_nt(a, b):
    return lax.dot_general(a, b, (((1,), (1,)), ((), ())), preferred_element_type=F32)


def kernel(tok, wg_hbm, wu_hbm, wd_hbm, out, wg_raw, wu_raw, wd_raw, wg, wu, wd, slab, x, pf, uf_s, uf_r, ue_s, ue_r, ul_s, ul_r,
           ux_s, ux_r, gx_s, gx_r, gf_s, gf_r, ge_s, ge_r, gl_s, gl_r, uk, hb, mf, dd_s, dd_r, mb, mr, own,
           wsem, t1s, t1r, zs, zr, rs, rr, ms, mrs):
    f = lax.axis_index("fs")
    t = lax.axis_index("tp")
    y, xl = f // 2, f % 2
    z, xh, core = t // 4, (t // 2) % 2, t % 2
    chip = t // 2
    ff = pf.shape[-1]

    def fs_dev(yy, xx):
        return {"fs": (yy % 4) * 2 + xx, "tp": t}

    def tp_dev(zz, hh, cc):
        return {"fs": f, "tp": (zz % 4) * 4 + hh * 2 + cc}

    loads = [pltpu.make_async_copy(a, b, wsem.at[i]) for i, (a, b) in enumerate(((wu_hbm, wu_raw), (wg_hbm, wg_raw), (wd_hbm, wd_raw)))]
    for c in loads:
        c.start()

    ydev = (fs_dev(y + 1, xl), fs_dev(y + 3, xl))
    xdev = fs_dev(y, 1 - xl)
    cdev = tp_dev(z, xh, 1 - core)
    zdev = (tp_dev(z + 1, xh, core), tp_dev(z + 3, xh, core))
    chips = [{"fs": f, "tp": ((chip + k) % 8) * 2 + core} for k in range(1, 8)]
    quarter = xh * 2 + core
    slot = quarter * 8 + f
    col = xh * 2 + xl
    hops = lambda n: min(n, 4 - n)
    near_last = sorted(((dy, dx, dc) for dy in range(4) for dx in range(4) for dc in range(2)), key=lambda o: -(hops(o[0]) + hops(o[1])))
    plane, owner = [], []
    for dy, dx, dc in near_last[:-2] + [(0, 0, 1)]:
        cx = (col + dx) % 4
        plane.append({"fs": ((y + dy) % 4) * 2 + cx % 2, "tp": z * 4 + (cx // 2) * 2 + (core + dc) % 2})
        owner.append(((y + dy) % 4) * 2 + cx % 2)

    barrier = pltpu.get_barrier_semaphore()
    peers = plane + list(zdev)
    for d in peers:
        pl.semaphore_signal(barrier, inc=1, device_id=d, device_id_type=MESH)
    pl.semaphore_wait(barrier, len(peers))

    sent = []

    def send(src, dst, ssem, rsem, dev):
        c = pltpu.make_async_remote_copy(src_ref=src, dst_ref=dst, send_sem=ssem, recv_sem=rsem, device_id=dev, device_id_type=MESH)
        c.start()
        sent.append(c)
        return c

    t1 = []
    for k in range(31):
        cols = pl.ds(pl.multiple_of(owner[k] * 1024, 1024), 1024)
        t1.append(send(tok.at[:, cols], slab.at[slot], t1s.at[k], t1r.at[k], plane[k]))
    slab[slot] = tok[:, pl.ds(pl.multiple_of(f * 1024, 1024), 1024)]
    for b in range(4):
        mr[b, chip] = jnp.zeros_like(mr[b, chip])
    loads[0].wait()
    wu[...] = wu_raw[...].T
    loads[1].wait()
    wg[...] = wg_raw[...].T

    zb = (z, (z + 3) % 4, (z + 1) % 4, (z + 2) % 4)
    r32 = lambda yy: pl.ds(pl.multiple_of((yy % 4) * 32, 32), 32)
    r16 = lambda yy, xx: pl.ds(pl.multiple_of((yy % 4) * 32 + xx * 16, 16), 16)
    zc = {}

    def zsend(k, block, start, rows, dev):
        part = x.at[block, pl.ds(pl.multiple_of(start, 32), rows)]
        zc[k] = send(part, part, zs.at[k], zr.at[k], dev)

    def first(_):
        for c in t1:
            c.wait_recv()
        x[z] = slab[...].astype(F32).reshape(128, 1024).astype(BF)
        for d in (0, 1):
            zsend(d, z, core * 64, 64, zdev[d])

    def relay(d):
        zc[d].wait_recv()
        zsend(2 + d, zb[1 + d], core * 64, 64, cdev)
        zsend(4 + d, zb[1 + d], core * 64 + 32 * d, 32, zdev[d])

    def relay_far(_):
        for d in (0, 1):
            zc[4 + d].wait_recv()
        zsend(6, zb[3], core * 64, 64, cdev)

    held = {0}

    def tokens(i):
        if i not in held:
            held.add(i)
            zc[(2, 3, 6)[i - 1]].wait_recv()

    def turn(_):
        loads[2].wait()
        wd[...] = wd_raw[...].T

    rc = {}

    def rsend(i, k, src, dst, dev):
        rc[i, k] = send(src, dst, rs.at[i, k], rr.at[i, k], dev)

    def near(d):
        return y + 1 + 2 * d

    lcol, rcol = pl.ds(0, GL_COLS), pl.ds(GL_COLS, ff - GL_COLS)
    gcol = (lcol, rcol)

    def up(i):
        tokens(i)
        pf[i, 1] = jnp.dot(x[zb[i]], wu[...], preferred_element_type=F32)
        for d in (0, 1):
            uf_s[i, d] = pf[i, 1, r16(y + 2, d), :].astype(BF)
            rsend(i, UF + d, uf_s.at[i, d], uf_r.at[i, d], ydev[d])
        for d in (0, 1):
            ue_s[i, d] = pf[i, 1, r16(near(d), 1 - d), :].astype(BF)
            rsend(i, UE + d, ue_s.at[i, d], ue_r.at[i, d], ydev[d])

    def gate(i):
        tokens(i)
        pf[i, 0] = jnp.dot(x[zb[i]], wg[...], preferred_element_type=F32)
        for k, j in enumerate((2, 1, 3, 0)):
            gx_s[i, k] = pf[i, 0, r16(y + j, 1 - xl), :].astype(BF)
            rsend(i, GX + k, gx_s.at[i, k], gx_r.at[i, k], xdev)

    def up_late(i):
        for d in (0, 1):
            rc[i, UF + d].wait_recv()
            ul_s[i, d] = (pf[i, 1, r16(near(d), d), :] + uf_r[i, d].astype(F32)).astype(BF)
            rsend(i, UL + d, ul_s.at[i, d], ul_r.at[i, d], ydev[d])

    def gate_far(i):
        rc[i, GX].wait_recv()
        gf_s[i] = (pf[i, 0, r16(y + 2, xl), :] + gx_r[i, 0].astype(F32)).astype(BF)
        for d in (0, 1):
            rsend(i, GF + d, gf_s.at[i, :, gcol[d]], gf_r.at[i, :, gcol[d]], ydev[d])
        for d in (0, 1):
            rc[i, GX + 1 + d].wait_recv()
            c = gcol[1 - d]
            ge_s[i, d, :, c] = (pf[i, 0, r16(near(d), xl), c] + gx_r[i, 1 + d, :, c].astype(F32)).astype(BF)
            rsend(i, GE + d, ge_s.at[i, d, :, c], ge_r.at[i, d, :, c], ydev[d])

    def up_pair(i):
        for k in (UE, UE + 1, UL, UL + 1):
            rc[i, k].wait_recv()
        s0 = pf[i, 1, r16(y, 0), :] + ul_r[i, 0].astype(F32) + ue_r[i, 1].astype(F32)
        s1 = pf[i, 1, r16(y, 1), :] + ue_r[i, 0].astype(F32) + ul_r[i, 1].astype(F32)
        ux_s[i] = jnp.where(xl == 0, s1, s0).astype(BF)
        rsend(i, UX, ux_s.at[i], ux_r.at[i], xdev)
        uk[i] = jnp.where(xl == 0, s0, s1)

    def gate_late(i):
        for d in (0, 1):
            rc[i, GF + d].wait_recv()
            c = gcol[d]
            gl_s[i, d, :, c] = (pf[i, 0, r16(near(d), xl), c] + gx_r[i, 1 + d, :, c].astype(F32) + gf_r[i, :, c].astype(F32)).astype(BF)
            rsend(i, GL + d, gl_s.at[i, d, :, c], gl_r.at[i, d, :, c], ydev[d])

    pcol, qcol = pl.ds(0, P_COLS), pl.ds(P_COLS, ff - P_COLS)
    qhalf = (pl.ds(P_COLS, Q_COLS - P_COLS), pl.ds(Q_COLS, ff - Q_COLS))

    def hid(i):
        for k in (GX + 3, GE, GE + 1, GL, GL + 1, UX):
            rc[i, k].wait_recv()
        u = uk[i] + ux_r[i].astype(F32)
        for d in (0, 1):
            c = gcol[d]
            g = pf[i, 0, r16(y, xl), c] + gx_r[i, 3, :, c].astype(F32) + gl_r[i, d, :, c].astype(F32) + ge_r[i, 1 - d, :, c].astype(F32)
            uc = u[:, :GL_COLS] if d == 0 else u[:, GL_COLS:]
            hb[i, r16(y, xl), c] = (g / (1.0 + jnp.exp(-g)) * uc).astype(BF)
        mine = r16(y, xl)
        p, q = hb.at[i, mine, pcol], hb.at[i, mine, qcol]
        rsend(i, AX, p, p, xdev)
        for d in (0, 1):
            rsend(i, AY + d, q, q, ydev[d])
        rsend(i, AR, q, q, xdev)

    def spread(i):
        rc[i, AX].wait_recv()
        pair = hb.at[i, r32(y), pcol]
        for d in (0, 1):
            rsend(i, AP + d, pair, pair, ydev[d])
        for d in (0, 1):
            rc[i, AY + d].wait_recv()
            row = r16(near(1 - d), xl)
            part, whole = hb.at[i, row, qhalf[d]], hb.at[i, row, qcol]
            rsend(i, AQ + d, part, part, ydev[d])
            rsend(i, AR + 1 + d, whole, whole, xdev)

    def spread_far(i):
        for d in (0, 1):
            rc[i, AP + d].wait_recv()
            part = hb.at[i, r16(near(1 - d), d), pcol]
            rsend(i, AF + d, part, part, ydev[d])
        for d in (0, 1):
            rc[i, AQ + d].wait_recv()
        whole = hb.at[i, r16(y + 2, xl), qcol]
        rsend(i, AR + 3, whole, whole, xdev)

    def arrived(i):
        for k in (AF, AF + 1, AR, AR + 1, AR + 2, AR + 3):
            rc[i, k].wait_recv()

    def halves(i):
        dd_s[i] = mf[i, :, 1 - core]
        rsend(i, DD, dd_s.at[i], dd_r.at[i], cdev)

    def down(i):
        arrived(i)
        mf[i] = dot_nt(wd[...], hb[i]).reshape(8, 2, 64, 128)
        halves(i)

    def down_two(i):
        arrived(i)
        arrived(i + 1)
        both = dot_nt(wd[...], hb[i : i + 2].reshape(256, ff))
        for j in (0, 1):
            mf[i + j] = both[:, j * 128 : (j + 1) * 128].reshape(8, 2, 64, 128)
            halves(i + j)

    mc = {}

    def columns(i):
        rc[i, DD].wait_recv()
        mf[i, :, core] = mf[i, :, core] + dd_r[i]
        mb[i] = mf[i, :, core].astype(BF)
        own[zb[i]] = mf[i, chip, core]
        for k in range(1, 8):
            g = (chip + k) % 8
            mc[i, k] = send(mb.at[i, g], mr.at[zb[i], chip], ms.at[i, k], mrs.at[zb[i], chip], chips[k - 1])

    def collect(b, m):
        g = (b * 2 + 4 + m) % 8

        @pl.when(g != chip)
        def _():
            pltpu.make_async_remote_copy(src_ref=mr.at[b, g], dst_ref=mr.at[b, g], send_sem=ms.at[b, 0], recv_sem=mrs.at[b, g],
                                         device_id=chips[0], device_id_type=MESH).wait_recv()

        return mr[b, g].astype(F32)

    ops = dict(t=first, r=relay, f=relay_far, w=turn, u=up, g=gate, b=up_late, c=gate_far, d=up_pair, e=gate_late, h=hid,
               i=spread, j=spread_far, k=down, K=down_two, l=columns)
    for step in " ".join(PLAN).split():
        ops[step[0]](int(step[1:]))

    for b in range(4):
        own[b] = own[b] + sum(collect(b, m) for m in range(2, 8))
    for b in range(4):
        out[:, b * 128 : (b + 1) * 128] = (own[b] + collect(b, 0) + collect(b, 1)).astype(BF)
    for c in sent:
        c.wait_send()


def body(tokens, gate_weight, up_weight, down_weight):
    d, ff = gate_weight.shape
    vm = pltpu.VMEM
    sem = lambda *s: pltpu.SemaphoreType.DMA(s) if s else pltpu.SemaphoreType.DMA
    piece = lambda: vm((4, 2, 16, ff), BF)
    one = lambda: vm((4, 16, ff), BF)
    scratch = [
        vm((ff, d), BF), vm((ff, d), BF), vm((ff, d), BF), vm((d, ff), BF), vm((d, ff), BF), vm((d, ff), BF), vm((32, 4, 1024), BF), vm((4, 128, 1024), BF),
        vm((4, 2, 128, ff), F32), piece(), piece(), piece(), piece(), piece(), piece(), one(), one(),
        vm((4, 4, 16, ff), BF), vm((4, 4, 16, ff), BF), one(), one(), piece(), piece(), piece(), piece(),
        vm((4, 16, ff), F32), vm((4, 128, ff), BF),
        vm((4, 8, 2, 64, 128), F32), vm((4, 8, 64, 128), F32), vm((4, 8, 64, 128), F32), vm((4, 8, 64, 128), BF),
        vm((4, 8, 64, 128), BF), vm((4, 64, 128), F32),
        sem(3), sem(31), sem(31), sem(7), sem(7), sem(4, 31), sem(4, 31), sem(4, 8), sem(4, 8),
    ]
    return pl.pallas_call(
        kernel,
        out_shape=jax.ShapeDtypeStruct((64, 512), BF),
        in_specs=[pl.BlockSpec(memory_space=vm)] + [pl.BlockSpec(memory_space=pl.ANY)] * 3,
        out_specs=pl.BlockSpec(memory_space=vm),
        scratch_shapes=scratch,
        compiler_params=pltpu.CompilerParams(collective_id=0, has_side_effects=True, vmem_limit_bytes=60 * 2**20),
        name="ffn",
    )(tokens, gate_weight.T, up_weight.T, down_weight).T


def solution(mesh):
    in_specs = (P(("tp", "fs"), None), P("fs", "tp"), P("fs", "tp"), P("tp", "fs"))
    out_specs = P(None, ("fs", "tp"))
    return jax.shard_map(body, mesh=mesh, in_specs=in_specs, out_specs=out_specs, check_vma=False)
```

```python
import functools

import jax
import jax.numpy as jnp
from jax import lax
from jax.experimental import pallas as pl
from jax.experimental.pallas import tpu as pltpu
from jax.sharding import PartitionSpec as P

BF = jnp.bfloat16
F32 = jnp.float32
MESH = pl.DeviceIdType.MESH

(UF, UE, UL, UX, GX, GF, GE, GL, AX, AY, AP, AQ, AF, AR, DD) = (0, 2, 4, 6, 7, 11, 13, 15, 17, 18, 20, 22, 24, 26, 30)
GL_COLS = 896
P_COLS = 1280
Q_COLS = 1536
PLAN = (
    "t0 g0 u0 r1",
    "r0 b0 g2 c0",
    "u1 f0 u2 g3",
    "d0 c2 w0 b1",
    "e0 g1 b2 u3",
    "e2 d2 b3 h0",
    "c3 c1 d1 e3",
    "h2 e1 d3 i0",
    "i2 h3 j0 h1",
    "j2 i3 i1 k2",
    "j3 k0 j1 l2",
    "l0 k3 k1 l3",
    "l1",
)


def dot_nt(a, b):
    return lax.dot_general(a, b, (((1,), (1,)), ((), ())), preferred_element_type=F32)


def kernel(tok_hbm, wg_hbm, wu_hbm, wd_hbm, out, tok, wg_raw, wu_raw, wd_raw, wg, wu, wd, slab, x, pf, uf_s, uf_r, ue_s, ue_r, ul_s, ul_r,
           ux_s, ux_r, gx_s, gx_r, gf_s, gf_r, ge_s, ge_r, gl_s, gl_r, uk, hb, mf, dd_s, dd_r, mb, mr, own,
           wsem, t1s, t1r, zs, zr, rs, rr, ms, mrs):
    f = lax.axis_index("fs")
    t = lax.axis_index("tp")
    y, xl = f // 2, f % 2
    z, xh, core = t // 4, (t // 2) % 2, t % 2
    chip = t // 2
    ff = pf.shape[-1]

    def fs_dev(yy, xx):
        return {"fs": (yy % 4) * 2 + xx, "tp": t}

    def tp_dev(zz, hh, cc):
        return {"fs": f, "tp": (zz % 4) * 4 + hh * 2 + cc}

    loads = [pltpu.make_async_copy(a, b, wsem.at[i]) for i, (a, b) in enumerate(((wu_hbm, wu_raw), (wg_hbm, wg_raw), (wd_hbm, wd_raw), (tok_hbm, tok)))]
    for k in (3, 0, 1, 2):
        loads[k].start()

    ydev = (fs_dev(y + 1, xl), fs_dev(y + 3, xl))
    xdev = fs_dev(y, 1 - xl)
    cdev = tp_dev(z, xh, 1 - core)
    zdev = (tp_dev(z + 1, xh, core), tp_dev(z + 3, xh, core))
    chips = [{"fs": f, "tp": ((chip + k) % 8) * 2 + core} for k in range(1, 8)]
    quarter = xh * 2 + core
    slot = quarter * 8 + f
    col = xh * 2 + xl
    hops = lambda n: min(n, 4 - n)
    near_last = sorted(((dy, dx, dc) for dy in range(4) for dx in range(4) for dc in range(2)), key=lambda o: -(hops(o[0]) + hops(o[1])))
    plane, owner = [], []
    for dy, dx, dc in near_last[:-2] + [(0, 0, 1)]:
        cx = (col + dx) % 4
        plane.append({"fs": ((y + dy) % 4) * 2 + cx % 2, "tp": z * 4 + (cx // 2) * 2 + (core + dc) % 2})
        owner.append(((y + dy) % 4) * 2 + cx % 2)

    barrier = pltpu.get_barrier_semaphore()
    peers = plane + list(zdev)
    for d in peers:
        pl.semaphore_signal(barrier, inc=1, device_id=d, device_id_type=MESH)
    pl.semaphore_wait(barrier, len(peers))

    sent = []

    def send(src, dst, ssem, rsem, dev):
        c = pltpu.make_async_remote_copy(src_ref=src, dst_ref=dst, send_sem=ssem, recv_sem=rsem, device_id=dev, device_id_type=MESH)
        c.start()
        sent.append(c)
        return c

    loads[3].wait()
    t1 = []
    for k in range(31):
        cols = pl.ds(pl.multiple_of(owner[k] * 1024, 1024), 1024)
        t1.append(send(tok.at[:, cols], slab.at[slot], t1s.at[k], t1r.at[k], plane[k]))
    slab[slot] = tok[:, pl.ds(pl.multiple_of(f * 1024, 1024), 1024)]
    for b in range(4):
        mr[b, chip] = jnp.zeros_like(mr[b, chip])
    loads[0].wait()
    wu[...] = wu_raw[...].T
    loads[1].wait()
    wg[...] = wg_raw[...].T

    zb = (z, (z + 3) % 4, (z + 1) % 4, (z + 2) % 4)
    r32 = lambda yy: pl.ds(pl.multiple_of((yy % 4) * 32, 32), 32)
    r16 = lambda yy, xx: pl.ds(pl.multiple_of((yy % 4) * 32 + xx * 16, 16), 16)
    zc = {}

    def zsend(k, block, start, rows, dev):
        part = x.at[block, pl.ds(pl.multiple_of(start, 32), rows)]
        zc[k] = send(part, part, zs.at[k], zr.at[k], dev)

    def first(_):
        for c in t1:
            c.wait_recv()
        x[z] = slab[...].astype(F32).reshape(128, 1024).astype(BF)
        for d in (0, 1):
            zsend(d, z, core * 64, 64, zdev[d])

    def relay(d):
        zc[d].wait_recv()
        zsend(2 + d, zb[1 + d], core * 64, 64, cdev)
        zsend(4 + d, zb[1 + d], core * 64 + 32 * d, 32, zdev[d])

    def relay_far(_):
        for d in (0, 1):
            zc[4 + d].wait_recv()
        zsend(6, zb[3], core * 64, 64, cdev)

    held = {0}

    def tokens(i):
        if i not in held:
            held.add(i)
            zc[(2, 3, 6)[i - 1]].wait_recv()

    def turn(_):
        loads[2].wait()
        wd[...] = wd_raw[...].T

    rc = {}

    def rsend(i, k, src, dst, dev):
        rc[i, k] = send(src, dst, rs.at[i, k], rr.at[i, k], dev)

    def near(d):
        return y + 1 + 2 * d

    lcol, rcol = pl.ds(0, GL_COLS), pl.ds(GL_COLS, ff - GL_COLS)
    gcol = (lcol, rcol)

    def up(i):
        tokens(i)
        pf[i, 1] = jnp.dot(x[zb[i]], wu[...], preferred_element_type=F32)
        for d in (0, 1):
            uf_s[i, d] = pf[i, 1, r16(y + 2, d), :].astype(BF)
            rsend(i, UF + d, uf_s.at[i, d], uf_r.at[i, d], ydev[d])
        for d in (0, 1):
            ue_s[i, d] = pf[i, 1, r16(near(d), 1 - d), :].astype(BF)
            rsend(i, UE + d, ue_s.at[i, d], ue_r.at[i, d], ydev[d])

    def gate(i):
        tokens(i)
        pf[i, 0] = jnp.dot(x[zb[i]], wg[...], preferred_element_type=F32)
        for k, j in enumerate((2, 1, 3, 0)):
            gx_s[i, k] = pf[i, 0, r16(y + j, 1 - xl), :].astype(BF)
            rsend(i, GX + k, gx_s.at[i, k], gx_r.at[i, k], xdev)

    def up_late(i):
        for d in (0, 1):
            rc[i, UF + d].wait_recv()
            ul_s[i, d] = (pf[i, 1, r16(near(d), d), :] + uf_r[i, d].astype(F32)).astype(BF)
            rsend(i, UL + d, ul_s.at[i, d], ul_r.at[i, d], ydev[d])

    def gate_far(i):
        rc[i, GX].wait_recv()
        gf_s[i] = (pf[i, 0, r16(y + 2, xl), :] + gx_r[i, 0].astype(F32)).astype(BF)
        for d in (0, 1):
            rsend(i, GF + d, gf_s.at[i, :, gcol[d]], gf_r.at[i, :, gcol[d]], ydev[d])
        for d in (0, 1):
            rc[i, GX + 1 + d].wait_recv()
            c = gcol[1 - d]
            ge_s[i, d, :, c] = (pf[i, 0, r16(near(d), xl), c] + gx_r[i, 1 + d, :, c].astype(F32)).astype(BF)
            rsend(i, GE + d, ge_s.at[i, d, :, c], ge_r.at[i, d, :, c], ydev[d])

    def up_pair(i):
        for k in (UE, UE + 1, UL, UL + 1):
            rc[i, k].wait_recv()
        s0 = pf[i, 1, r16(y, 0), :] + ul_r[i, 0].astype(F32) + ue_r[i, 1].astype(F32)
        s1 = pf[i, 1, r16(y, 1), :] + ue_r[i, 0].astype(F32) + ul_r[i, 1].astype(F32)
        ux_s[i] = jnp.where(xl == 0, s1, s0).astype(BF)
        rsend(i, UX, ux_s.at[i], ux_r.at[i], xdev)
        uk[i] = jnp.where(xl == 0, s0, s1)

    def gate_late(i):
        for d in (0, 1):
            rc[i, GF + d].wait_recv()
            c = gcol[d]
            gl_s[i, d, :, c] = (pf[i, 0, r16(near(d), xl), c] + gx_r[i, 1 + d, :, c].astype(F32) + gf_r[i, :, c].astype(F32)).astype(BF)
            rsend(i, GL + d, gl_s.at[i, d, :, c], gl_r.at[i, d, :, c], ydev[d])

    pcol, qcol = pl.ds(0, P_COLS), pl.ds(P_COLS, ff - P_COLS)
    qhalf = (pl.ds(P_COLS, Q_COLS - P_COLS), pl.ds(Q_COLS, ff - Q_COLS))

    def hid(i):
        for k in (GX + 3, GE, GE + 1, GL, GL + 1, UX):
            rc[i, k].wait_recv()
        u = uk[i] + ux_r[i].astype(F32)
        for d in (0, 1):
            c = gcol[d]
            g = pf[i, 0, r16(y, xl), c] + gx_r[i, 3, :, c].astype(F32) + gl_r[i, d, :, c].astype(F32) + ge_r[i, 1 - d, :, c].astype(F32)
            uc = u[:, :GL_COLS] if d == 0 else u[:, GL_COLS:]
            hb[i, r16(y, xl), c] = (g / (1.0 + jnp.exp(-g)) * uc).astype(BF)
        mine = r16(y, xl)
        p, q = hb.at[i, mine, pcol], hb.at[i, mine, qcol]
        rsend(i, AX, p, p, xdev)
        for d in (0, 1):
            rsend(i, AY + d, q, q, ydev[d])
        rsend(i, AR, q, q, xdev)

    def spread(i):
        rc[i, AX].wait_recv()
        pair = hb.at[i, r32(y), pcol]
        for d in (0, 1):
            rsend(i, AP + d, pair, pair, ydev[d])
        for d in (0, 1):
            rc[i, AY + d].wait_recv()
            row = r16(near(1 - d), xl)
            part, whole = hb.at[i, row, qhalf[d]], hb.at[i, row, qcol]
            rsend(i, AQ + d, part, part, ydev[d])
            rsend(i, AR + 1 + d, whole, whole, xdev)

    def spread_far(i):
        for d in (0, 1):
            rc[i, AP + d].wait_recv()
            part = hb.at[i, r16(near(1 - d), d), pcol]
            rsend(i, AF + d, part, part, ydev[d])
        for d in (0, 1):
            rc[i, AQ + d].wait_recv()
        whole = hb.at[i, r16(y + 2, xl), qcol]
        rsend(i, AR + 3, whole, whole, xdev)

    def arrived(i):
        for k in (AF, AF + 1, AR, AR + 1, AR + 2, AR + 3):
            rc[i, k].wait_recv()

    def halves(i):
        dd_s[i] = mf[i, :, 1 - core]
        rsend(i, DD, dd_s.at[i], dd_r.at[i], cdev)

    def down(i):
        arrived(i)
        mf[i] = dot_nt(wd[...], hb[i]).reshape(8, 2, 64, 128)
        halves(i)

    def down_two(i):
        arrived(i)
        arrived(i + 1)
        both = dot_nt(wd[...], hb[i : i + 2].reshape(256, ff))
        for j in (0, 1):
            mf[i + j] = both[:, j * 128 : (j + 1) * 128].reshape(8, 2, 64, 128)
            halves(i + j)

    mc = {}

    def columns(i):
        rc[i, DD].wait_recv()
        mf[i, :, core] = mf[i, :, core] + dd_r[i]
        mb[i] = mf[i, :, core].astype(BF)
        own[zb[i]] = mf[i, chip, core]
        for k in range(1, 8):
            g = (chip + k) % 8
            mc[i, k] = send(mb.at[i, g], mr.at[zb[i], chip], ms.at[i, k], mrs.at[zb[i], chip], chips[k - 1])

    def collect(b, m):
        g = (b * 2 + 4 + m) % 8

        @pl.when(g != chip)
        def _():
            pltpu.make_async_remote_copy(src_ref=mr.at[b, g], dst_ref=mr.at[b, g], send_sem=ms.at[b, 0], recv_sem=mrs.at[b, g],
                                         device_id=chips[0], device_id_type=MESH).wait_recv()

        return mr[b, g].astype(F32)

    ops = dict(t=first, r=relay, f=relay_far, w=turn, u=up, g=gate, b=up_late, c=gate_far, d=up_pair, e=gate_late, h=hid,
               i=spread, j=spread_far, k=down, K=down_two, l=columns)
    for step in " ".join(PLAN).split():
        ops[step[0]](int(step[1:]))

    for b in range(4):
        own[b] = own[b] + sum(collect(b, m) for m in range(2, 8))
    for b in range(4):
        out[:, b * 128 : (b + 1) * 128] = (own[b] + collect(b, 0) + collect(b, 1)).astype(BF)
    for c in sent:
        c.wait_send()


def body(tokens, gate_weight, up_weight, down_weight):
    d, ff = gate_weight.shape
    vm = pltpu.VMEM
    sem = lambda *s: pltpu.SemaphoreType.DMA(s) if s else pltpu.SemaphoreType.DMA
    piece = lambda: vm((4, 2, 16, ff), BF)
    one = lambda: vm((4, 16, ff), BF)
    scratch = [
        vm((4, 8192), BF), vm((ff, d), BF), vm((ff, d), BF), vm((ff, d), BF), vm((d, ff), BF), vm((d, ff), BF), vm((d, ff), BF), vm((32, 4, 1024), BF), vm((4, 128, 1024), BF),
        vm((4, 2, 128, ff), F32), piece(), piece(), piece(), piece(), piece(), piece(), one(), one(),
        vm((4, 4, 16, ff), BF), vm((4, 4, 16, ff), BF), one(), one(), piece(), piece(), piece(), piece(),
        vm((4, 16, ff), F32), vm((4, 128, ff), BF),
        vm((4, 8, 2, 64, 128), F32), vm((4, 8, 64, 128), F32), vm((4, 8, 64, 128), F32), vm((4, 8, 64, 128), BF),
        vm((4, 8, 64, 128), BF), vm((4, 64, 128), F32),
        sem(4), sem(31), sem(31), sem(7), sem(7), sem(4, 31), sem(4, 31), sem(4, 8), sem(4, 8),
    ]
    return pl.pallas_call(
        kernel,
        out_shape=jax.ShapeDtypeStruct((64, 512), BF),
        in_specs=[pl.BlockSpec(memory_space=pl.ANY)] * 4,
        out_specs=pl.BlockSpec(memory_space=vm),
        scratch_shapes=scratch,
        compiler_params=pltpu.CompilerParams(collective_id=0, has_side_effects=True, vmem_limit_bytes=52 * 2**20),
        name="ffn",
    )(tokens, gate_weight.T, up_weight.T, down_weight).T


def solution(mesh):
    in_specs = (P(("tp", "fs"), None), P("fs", "tp"), P("fs", "tp"), P("tp", "fs"))
    out_specs = P(None, ("fs", "tp"))
    return jax.shard_map(body, mesh=mesh, in_specs=in_specs, out_specs=out_specs, check_vma=False)
```

```python
import functools

import jax
import jax.numpy as jnp
from jax import lax
from jax.experimental import pallas as pl
from jax.experimental.pallas import tpu as pltpu
from jax.sharding import PartitionSpec as P

BF = jnp.bfloat16
F32 = jnp.float32
MESH = pl.DeviceIdType.MESH

(UF, UE, UL, UX, GX, GF, GE, GL, AX, AY, AP, AQ, AF, AR, DD) = (0, 2, 4, 6, 7, 11, 13, 15, 17, 18, 20, 22, 24, 26, 30)
GL_COLS = 896
P_COLS = 1280
Q_COLS = 1536
PLAN = (
    "t0 g0 u0 r1",
    "g2 b0 c0 r0",
    "u2 g1 f0 e0",
    "c2 d0 b2 u1",
    "g3 u3 d2 b1",
    "e2 c1 h0 b3",
    "d1 c3 e1 h2",
    "i0 e3 d3 h1",
    "i2 j0 h3 i1",
    "j2 i3 w0 k0",
    "j1 k2 j3 l2",
    "l0 k1 k3 l1",
    "l3",
)


def dot_nt(a, b):
    return lax.dot_general(a, b, (((1,), (1,)), ((), ())), preferred_element_type=F32)


def kernel(tok_hbm, wg_hbm, wu_hbm, wd_hbm, out, tok, wg_raw, wu_raw, wd_raw, wg, wu, wd, slab, x, pf, uf_s, uf_r, ue_s, ue_r, ul_s, ul_r,
           ux_s, ux_r, gx_s, gx_r, gf_s, gf_r, ge_s, ge_r, gl_s, gl_r, uk, hb, mf, dd_s, dd_r, mb, mr, own,
           wsem, t1s, t1r, zs, zr, rs, rr, ms, mrs):
    f = lax.axis_index("fs")
    t = lax.axis_index("tp")
    y, xl = f // 2, f % 2
    z, xh, core = t // 4, (t // 2) % 2, t % 2
    chip = t // 2
    ff = pf.shape[-1]

    def fs_dev(yy, xx):
        return {"fs": (yy % 4) * 2 + xx, "tp": t}

    def tp_dev(zz, hh, cc):
        return {"fs": f, "tp": (zz % 4) * 4 + hh * 2 + cc}

    loads = [pltpu.make_async_copy(a, b, wsem.at[i]) for i, (a, b) in enumerate(((wu_hbm, wu_raw), (wg_hbm, wg_raw), (wd_hbm, wd_raw), (tok_hbm, tok)))]
    for k in (3, 0, 1, 2):
        loads[k].start()

    ydev = (fs_dev(y + 1, xl), fs_dev(y + 3, xl))
    xdev = fs_dev(y, 1 - xl)
    cdev = tp_dev(z, xh, 1 - core)
    zdev = (tp_dev(z + 1, xh, core), tp_dev(z + 3, xh, core))
    chips = [{"fs": f, "tp": ((chip + k) % 8) * 2 + core} for k in range(1, 8)]
    quarter = xh * 2 + core
    slot = quarter * 8 + f
    col = xh * 2 + xl
    hops = lambda n: min(n, 4 - n)
    near_last = sorted(((dy, dx, dc) for dy in range(4) for dx in range(4) for dc in range(2)), key=lambda o: -(hops(o[0]) + hops(o[1])))
    plane, owner = [], []
    for dy, dx, dc in near_last[:-2] + [(0, 0, 1)]:
        cx = (col + dx) % 4
        plane.append({"fs": ((y + dy) % 4) * 2 + cx % 2, "tp": z * 4 + (cx // 2) * 2 + (core + dc) % 2})
        owner.append(((y + dy) % 4) * 2 + cx % 2)

    barrier = pltpu.get_barrier_semaphore()
    peers = plane + list(zdev)
    for d in peers:
        pl.semaphore_signal(barrier, inc=1, device_id=d, device_id_type=MESH)
    pl.semaphore_wait(barrier, len(peers))

    sent = []

    def send(src, dst, ssem, rsem, dev):
        c = pltpu.make_async_remote_copy(src_ref=src, dst_ref=dst, send_sem=ssem, recv_sem=rsem, device_id=dev, device_id_type=MESH)
        c.start()
        sent.append(c)
        return c

    loads[3].wait()
    t1 = []
    for k in range(31):
        cols = pl.ds(pl.multiple_of(owner[k] * 1024, 1024), 1024)
        t1.append(send(tok.at[:, cols], slab.at[slot], t1s.at[k], t1r.at[k], plane[k]))
    slab[slot] = tok[:, pl.ds(pl.multiple_of(f * 1024, 1024), 1024)]
    for b in range(4):
        mr[b, chip] = jnp.zeros_like(mr[b, chip])
    loads[0].wait()
    wu[...] = wu_raw[...].T
    loads[1].wait()
    wg[...] = wg_raw[...].T

    zb = (z, (z + 3) % 4, (z + 1) % 4, (z + 2) % 4)
    r32 = lambda yy: pl.ds(pl.multiple_of((yy % 4) * 32, 32), 32)
    r16 = lambda yy, xx: pl.ds(pl.multiple_of((yy % 4) * 32 + xx * 16, 16), 16)
    zc = {}

    def zsend(k, block, start, rows, dev):
        part = x.at[block, pl.ds(pl.multiple_of(start, 32), rows)]
        zc[k] = send(part, part, zs.at[k], zr.at[k], dev)

    def first(_):
        for c in t1:
            c.wait_recv()
        x[z] = slab[...].astype(F32).reshape(128, 1024).astype(BF)
        for d in (0, 1):
            zsend(d, z, core * 64, 64, zdev[d])

    def relay(d):
        zc[d].wait_recv()
        zsend(2 + d, zb[1 + d], core * 64, 64, cdev)
        zsend(4 + d, zb[1 + d], core * 64 + 32 * d, 32, zdev[d])

    def relay_far(_):
        for d in (0, 1):
            zc[4 + d].wait_recv()
        zsend(6, zb[3], core * 64, 64, cdev)

    held = {0}

    def tokens(i):
        if i not in held:
            held.add(i)
            zc[(2, 3, 6)[i - 1]].wait_recv()

    def turn(_):
        loads[2].wait()
        wd[...] = wd_raw[...].T

    rc = {}

    def rsend(i, k, src, dst, dev):
        rc[i, k] = send(src, dst, rs.at[i, k], rr.at[i, k], dev)

    def near(d):
        return y + 1 + 2 * d

    lcol, rcol = pl.ds(0, GL_COLS), pl.ds(GL_COLS, ff - GL_COLS)
    gcol = (lcol, rcol)

    def up(i):
        tokens(i)
        pf[i, 1] = jnp.dot(x[zb[i]], wu[...], preferred_element_type=F32)
        for d in (0, 1):
            uf_s[i, d] = pf[i, 1, r16(y + 2, d), :].astype(BF)
            rsend(i, UF + d, uf_s.at[i, d], uf_r.at[i, d], ydev[d])
        for d in (0, 1):
            ue_s[i, d] = pf[i, 1, r16(near(d), 1 - d), :].astype(BF)
            rsend(i, UE + d, ue_s.at[i, d], ue_r.at[i, d], ydev[d])

    def gate(i):
        tokens(i)
        pf[i, 0] = jnp.dot(x[zb[i]], wg[...], preferred_element_type=F32)
        for k, j in enumerate((2, 1, 3, 0)):
            gx_s[i, k] = pf[i, 0, r16(y + j, 1 - xl), :].astype(BF)
            rsend(i, GX + k, gx_s.at[i, k], gx_r.at[i, k], xdev)

    def up_late(i):
        for d in (0, 1):
            rc[i, UF + d].wait_recv()
            ul_s[i, d] = (pf[i, 1, r16(near(d), d), :] + uf_r[i, d].astype(F32)).astype(BF)
            rsend(i, UL + d, ul_s.at[i, d], ul_r.at[i, d], ydev[d])

    def gate_far(i):
        rc[i, GX].wait_recv()
        gf_s[i] = (pf[i, 0, r16(y + 2, xl), :] + gx_r[i, 0].astype(F32)).astype(BF)
        for d in (0, 1):
            rsend(i, GF + d, gf_s.at[i, :, gcol[d]], gf_r.at[i, :, gcol[d]], ydev[d])
        for d in (0, 1):
            rc[i, GX + 1 + d].wait_recv()
            c = gcol[1 - d]
            ge_s[i, d, :, c] = (pf[i, 0, r16(near(d), xl), c] + gx_r[i, 1 + d, :, c].astype(F32)).astype(BF)
            rsend(i, GE + d, ge_s.at[i, d, :, c], ge_r.at[i, d, :, c], ydev[d])

    def up_pair(i):
        for k in (UE, UE + 1, UL, UL + 1):
            rc[i, k].wait_recv()
        s0 = pf[i, 1, r16(y, 0), :] + ul_r[i, 0].astype(F32) + ue_r[i, 1].astype(F32)
        s1 = pf[i, 1, r16(y, 1), :] + ue_r[i, 0].astype(F32) + ul_r[i, 1].astype(F32)
        ux_s[i] = jnp.where(xl == 0, s1, s0).astype(BF)
        rsend(i, UX, ux_s.at[i], ux_r.at[i], xdev)
        uk[i] = jnp.where(xl == 0, s0, s1)

    def gate_late(i):
        for d in (0, 1):
            rc[i, GF + d].wait_recv()
            c = gcol[d]
            gl_s[i, d, :, c] = (pf[i, 0, r16(near(d), xl), c] + gx_r[i, 1 + d, :, c].astype(F32) + gf_r[i, :, c].astype(F32)).astype(BF)
            rsend(i, GL + d, gl_s.at[i, d, :, c], gl_r.at[i, d, :, c], ydev[d])

    pcol, qcol = pl.ds(0, P_COLS), pl.ds(P_COLS, ff - P_COLS)
    qhalf = (pl.ds(P_COLS, Q_COLS - P_COLS), pl.ds(Q_COLS, ff - Q_COLS))

    def hid(i):
        for k in (GX + 3, GE, GE + 1, GL, GL + 1, UX):
            rc[i, k].wait_recv()
        u = uk[i] + ux_r[i].astype(F32)
        for d in (0, 1):
            c = gcol[d]
            g = pf[i, 0, r16(y, xl), c] + gx_r[i, 3, :, c].astype(F32) + gl_r[i, d, :, c].astype(F32) + ge_r[i, 1 - d, :, c].astype(F32)
            uc = u[:, :GL_COLS] if d == 0 else u[:, GL_COLS:]
            hb[i, r16(y, xl), c] = (g / (1.0 + jnp.exp(-g)) * uc).astype(BF)
        mine = r16(y, xl)
        p, q = hb.at[i, mine, pcol], hb.at[i, mine, qcol]
        rsend(i, AX, p, p, xdev)
        for d in (0, 1):
            rsend(i, AY + d, q, q, ydev[d])
        rsend(i, AR, q, q, xdev)

    def spread(i):
        rc[i, AX].wait_recv()
        pair = hb.at[i, r32(y), pcol]
        for d in (0, 1):
            rsend(i, AP + d, pair, pair, ydev[d])
        for d in (0, 1):
            rc[i, AY + d].wait_recv()
            row = r16(near(1 - d), xl)
            part, whole = hb.at[i, row, qhalf[d]], hb.at[i, row, qcol]
            rsend(i, AQ + d, part, part, ydev[d])
            rsend(i, AR + 1 + d, whole, whole, xdev)

    def spread_far(i):
        for d in (0, 1):
            rc[i, AP + d].wait_recv()
            part = hb.at[i, r16(near(1 - d), d), pcol]
            rsend(i, AF + d, part, part, ydev[d])
        for d in (0, 1):
            rc[i, AQ + d].wait_recv()
        whole = hb.at[i, r16(y + 2, xl), qcol]
        rsend(i, AR + 3, whole, whole, xdev)

    def arrived(i):
        for k in (AF, AF + 1, AR, AR + 1, AR + 2, AR + 3):
            rc[i, k].wait_recv()

    def halves(i):
        dd_s[i] = mf[i, :, 1 - core]
        rsend(i, DD, dd_s.at[i], dd_r.at[i], cdev)

    def down(i):
        arrived(i)
        mf[i] = dot_nt(wd[...], hb[i]).reshape(8, 2, 64, 128)
        halves(i)

    def down_two(i):
        arrived(i)
        arrived(i + 1)
        both = dot_nt(wd[...], hb[i : i + 2].reshape(256, ff))
        for j in (0, 1):
            mf[i + j] = both[:, j * 128 : (j + 1) * 128].reshape(8, 2, 64, 128)
            halves(i + j)

    mc = {}

    def columns(i):
        rc[i, DD].wait_recv()
        mf[i, :, core] = mf[i, :, core] + dd_r[i]
        mb[i] = mf[i, :, core].astype(BF)
        own[zb[i]] = mf[i, chip, core]
        for k in range(1, 8):
            g = (chip + k) % 8
            mc[i, k] = send(mb.at[i, g], mr.at[zb[i], chip], ms.at[i, k], mrs.at[zb[i], chip], chips[k - 1])

    def collect(b, m):
        g = (b * 2 + 4 + m) % 8

        @pl.when(g != chip)
        def _():
            pltpu.make_async_remote_copy(src_ref=mr.at[b, g], dst_ref=mr.at[b, g], send_sem=ms.at[b, 0], recv_sem=mrs.at[b, g],
                                         device_id=chips[0], device_id_type=MESH).wait_recv()

        return mr[b, g].astype(F32)

    ops = dict(t=first, r=relay, f=relay_far, w=turn, u=up, g=gate, b=up_late, c=gate_far, d=up_pair, e=gate_late, h=hid,
               i=spread, j=spread_far, k=down, K=down_two, l=columns)
    for step in " ".join(PLAN).split():
        ops[step[0]](int(step[1:]))

    for b in range(4):
        own[b] = own[b] + sum(collect(b, m) for m in range(2, 8))
    for b in range(4):
        out[:, b * 128 : (b + 1) * 128] = (own[b] + collect(b, 0) + collect(b, 1)).astype(BF)
    for c in sent:
        c.wait_send()


def body(tokens, gate_weight, up_weight, down_weight):
    d, ff = gate_weight.shape
    vm = pltpu.VMEM
    sem = lambda *s: pltpu.SemaphoreType.DMA(s) if s else pltpu.SemaphoreType.DMA
    piece = lambda: vm((4, 2, 16, ff), BF)
    one = lambda: vm((4, 16, ff), BF)
    scratch = [
        vm((4, 8192), BF), vm((ff, d), BF), vm((ff, d), BF), vm((ff, d), BF), vm((d, ff), BF), vm((d, ff), BF), vm((d, ff), BF), vm((32, 4, 1024), BF), vm((4, 128, 1024), BF),
        vm((4, 2, 128, ff), F32), piece(), piece(), piece(), piece(), piece(), piece(), one(), one(),
        vm((4, 4, 16, ff), BF), vm((4, 4, 16, ff), BF), one(), one(), piece(), piece(), piece(), piece(),
        vm((4, 16, ff), F32), vm((4, 128, ff), BF),
        vm((4, 8, 2, 64, 128), F32), vm((4, 8, 64, 128), F32), vm((4, 8, 64, 128), F32), vm((4, 8, 64, 128), BF),
        vm((4, 8, 64, 128), BF), vm((4, 64, 128), F32),
        sem(4), sem(31), sem(31), sem(7), sem(7), sem(4, 31), sem(4, 31), sem(4, 8), sem(4, 8),
    ]
    return pl.pallas_call(
        kernel,
        out_shape=jax.ShapeDtypeStruct((64, 512), BF),
        in_specs=[pl.BlockSpec(memory_space=pl.ANY)] * 4,
        out_specs=pl.BlockSpec(memory_space=vm),
        scratch_shapes=scratch,
        compiler_params=pltpu.CompilerParams(collective_id=0, has_side_effects=True, vmem_limit_bytes=52 * 2**20),
        name="ffn",
    )(tokens, gate_weight.T, up_weight.T, down_weight).T


def solution(mesh):
    in_specs = (P(("tp", "fs"), None), P("fs", "tp"), P("fs", "tp"), P("tp", "fs"))
    out_specs = P(None, ("fs", "tp"))
    return jax.shard_map(body, mesh=mesh, in_specs=in_specs, out_specs=out_specs, check_vma=False)
```
